32 devices in a mesh: tok: 4 (over y, x), hid: 8 (over z, core).
Axes of the slice: x: 2, y: 2, z: 4, core: 2. Of those that a mesh axis runs over, the one named last changes fastest.
Arguments:
- tokens: bfloat16 [6144, 6144], P('tok', 'hid'), may hold values from -6 to 6
- cotangent: bfloat16 [6144, 6144], P('tok', 'hid'), may hold values from -6 to 6
- expert_choice: int32 [6144, 2], P('tok'), may hold values from 0 to 7, as said below
- router: bfloat16 [8, 6144], replicated, may hold values from -0.078125 to 0.078125
- gate_up: bfloat16 [6144, 2, 8192], P('tok', None, 'hid'), may hold values from -0.109375 to 0.109375
- w_down: bfloat16 [6144, 8192], P('tok', 'hid'), may hold values from -0.0625 to 0.0625
Outputs:
- grad_tokens: bfloat16 [6144, 6144], P('tok', 'hid')
- d_combine: float32 [6144, 2], P('tok')
- d_gate_up: float32 [6144, 2, 8192], P('tok', None, 'hid')
- d_down: float32 [6144, 8192], P('tok', 'hid')
The draws below stay inside these ranges and needn't reach their ends.
Inputs may be any that keep to these rules, and one draw needn't show every extreme that they name: `expert_choice`: each row names 2 different experts. In every aligned block of 1536 rows at most 432 rows name expert 0 and at least half of 432 do; some block has exactly 432.
All inputs are finite; a program needn't handle non-finite values.
Results may differ from the reference program's by a relative error of at most 0.017.
Values may be sent and summed in bfloat16 or wider, within the bound.
A program may use at most 128 MiB of HBM per device.

```python
import jax
import jax.numpy as jnp
from jax import lax

D = 6144
FF = 8192
EXPERTS = 8
TOK_GROUP = 1536
CAP = 432
TOKENS = 6144
N_TOK = 4


def draw_expert_choice(key, part):
    streams = jax.random.split(jax.random.fold_in(key, 17), 6)
    blocks = TOKENS // TOK_GROUP
    counts = jax.random.randint(streams[0], (blocks,), CAP // 2, CAP + 1)
    fullest = jax.random.randint(streams[1], (), 0, blocks)
    counts = jnp.where(jnp.arange(blocks) == fullest, CAP, counts)
    orders = jax.vmap(lambda block_key: jax.random.permutation(block_key, TOK_GROUP))(jax.random.split(streams[2], blocks))
    chosen = (orders < counts[:, None]).reshape(TOKENS)
    leading = jax.random.randint(streams[3], (TOKENS,), 1, EXPERTS)
    offset = jax.random.randint(streams[4], (TOKENS,), 1, EXPERTS - 1)
    trailing = 1 + (leading - 1 + offset) % (EXPERTS - 1)
    column = jax.random.randint(streams[5], (TOKENS,), 0, 2)
    left_entry = jnp.where(chosen, jnp.where(column == 0, 0, leading), leading)
    right_entry = jnp.where(chosen, jnp.where(column == 0, leading, 0), trailing)
    return jnp.stack([left_entry, right_entry], axis=1).astype(jnp.int32)


def raised(result, key, source, target, shards_of, factor):
    owner, partner = [(jnp.arange(result.shape[position]) // (result.shape[position] // shards_of)).reshape([-1 if axis == position else 1 for axis in range(result.ndim)]) for position in (source, target)]
    chosen = jax.random.permutation(key, shards_of)[partner]
    strong = (owner == chosen) | (owner == (partner + shards_of // 2) % shards_of)
    return jnp.where(strong, factor * result, result)


def levels(rng, dims, pieces, low, high):
    def one(axis_at, blocks):
        steps = jax.random.uniform(jax.random.fold_in(jax.random.fold_in(rng, 6), axis_at), (blocks,), jnp.float32, low / len(pieces), high / len(pieces))
        return jnp.repeat(jnp.exp(steps), dims[axis_at] // blocks).reshape((-1,) + (1,) * (len(dims) - axis_at - 1))

    gain = one(*pieces[0])
    for cut in pieces[1:]:
        gain = gain * one(*cut)
    return gain


def normal_values(key, shape, width, bound, cuts=(), kind=jnp.bfloat16):
    entries = width * jax.random.normal(key, shape, jnp.float32)
    if cuts:
        entries = entries * levels(key, shape, cuts, -0.22, 0.18)
    return jnp.clip(entries, -bound, bound).astype(kind)


def noise_with(rng, shape, deviation, bound, cuts, heavy, kind=jnp.bfloat16):
    drawn = deviation * jax.random.normal(rng, shape, jnp.float32)
    if cuts:
        drawn = drawn * levels(rng, shape, cuts, -0.22, 0.18)
    return jnp.clip(raised(drawn, jax.random.fold_in(rng, 3), *heavy), -bound, bound).astype(kind)


def setup_inputs(seed: int = 0) -> dict:
    seeds = jax.random.split(jax.random.key(seed), 7)
    tokens = noise_with(seeds[0], (TOKENS, D), 1.0, 6.0, ((0, 4), (1, 8)), (0, 1, 8, 2.0))
    cotangent = noise_with(seeds[1], (TOKENS, D), 1.0, 6.0, ((0, 4), (1, 8)), (0, 1, 8, 2.0))
    expert_choice = draw_expert_choice(jax.random.fold_in(seeds[6], 71), 0)
    router = normal_values(seeds[3], (EXPERTS, D), D ** -0.5, 0.078125)
    gate_up = noise_with(seeds[4], (D, 2, FF), D ** -0.5, 0.109375, ((0, 4), (2, 8)), (2, 0, 8, 2.0))
    w_down = normal_values(seeds[5], (D, FF), FF ** -0.5, 0.0625, ((0, 4), (1, 8)))
    return dict(tokens=tokens, cotangent=cotangent, expert_choice=expert_choice, router=router, gate_up=gate_up, w_down=w_down)


def silu_pair(pre):
    sigma = jax.nn.sigmoid(pre)
    return pre * sigma, sigma * (1.0 + pre * (1.0 - sigma))


def rounded_add(total, term):
    return total + lax.optimization_barrier(term.astype(jnp.bfloat16)).astype(jnp.float32)


def reference(tokens, cotangent, expert_choice, router, gate_up, w_down):
    logits = jnp.dot(tokens, router.T, preferred_element_type=jnp.float32)
    first = expert_choice[:, 0]
    second = expert_choice[:, 1]
    in_first = first == 0
    in_second = second == 0
    routed = jnp.logical_or(in_first, in_second)
    other = first + second
    labels = jnp.arange(EXPERTS, dtype=jnp.int32)
    other_logit = jnp.sum(jnp.where(other[:, None] == labels[None, :], logits, 0.0), axis=1)
    gating = jnp.where(routed, jax.nn.sigmoid(logits[:, 0] - other_logit), 0.0)
    flags = routed.astype(jnp.int32).reshape(N_TOK, TOK_GROUP)
    slot_rank = jnp.cumsum(flags, axis=1) - flags
    slot_ids = jnp.arange(CAP, dtype=jnp.int32)
    placed = jnp.logical_and(flags[:, None, :] > 0, slot_rank[:, None, :] == slot_ids[None, :, None])
    dispatch = placed.astype(jnp.float32)
    grouped_in = tokens.astype(jnp.float32).reshape(N_TOK, TOK_GROUP, D)
    grouped_cot = cotangent.astype(jnp.float32).reshape(N_TOK, TOK_GROUP, D)
    expert_in = jnp.einsum("kcr,krd->kcd", dispatch, grouped_in, precision=lax.Precision.HIGHEST).astype(jnp.bfloat16)
    expert_cot = jnp.einsum("kcr,krd->kcd", dispatch, grouped_cot, precision=lax.Precision.HIGHEST).astype(jnp.bfloat16)
    slot_gate = jnp.sum(dispatch * gating.reshape(N_TOK, 1, TOK_GROUP), axis=2)
    weights_in = gate_up.reshape(D, 2 * FF)
    grad_in = jnp.zeros((D, 2 * FF), jnp.float32)
    grad_out = jnp.zeros((D, FF), jnp.float32)
    back_rows = []
    score_rows = []
    for group in range(N_TOK):
        rows_in = expert_in[group]
        rows_cot = expert_cot[group]
        scale = slot_gate[group][:, None]
        joined = jnp.dot(rows_in, weights_in, preferred_element_type=jnp.float32)
        gate_pre = joined[:, :FF]
        up_pre = joined[:, FF:]
        raw = jnp.dot(rows_cot, w_down, preferred_element_type=jnp.float32)
        active, slope = silu_pair(gate_pre)
        product = active * up_pre
        scaled = (scale * product).astype(jnp.bfloat16)
        score_rows.append(jnp.sum(product * raw, axis=1))
        upstream = scale * raw
        grads_mid = jnp.concatenate([(upstream * up_pre * slope).astype(jnp.bfloat16), (upstream * active).astype(jnp.bfloat16)], axis=1)
        grad_in = rounded_add(grad_in, jnp.dot(rows_in.T, grads_mid, preferred_element_type=jnp.float32))
        grad_out = rounded_add(grad_out, jnp.dot(rows_cot.T, scaled, preferred_element_type=jnp.float32))
        back_rows.append(jnp.dot(grads_mid, weights_in.T, preferred_element_type=jnp.float32))
    back = jnp.stack(back_rows)
    scores = jnp.stack(score_rows)
    safe = jnp.minimum(slot_rank, CAP - 1).astype(jnp.int32)
    picked = jax.vmap(lambda rows, index: jnp.take(rows, index, axis=0))(back, safe).reshape(TOKENS, D)
    routed_flat = flags.reshape(TOKENS) > 0
    grad_tokens = jnp.where(routed_flat[:, None], picked, 0.0).astype(jnp.bfloat16)
    picked_score = jax.vmap(lambda rows, index: jnp.take(rows, index, axis=0))(scores, safe).reshape(TOKENS)
    token_score = jnp.where(routed, picked_score, 0.0)
    d_combine = jnp.stack([jnp.where(in_first, token_score, 0.0), jnp.where(in_second, token_score, 0.0)], axis=1)
    return grad_tokens, d_combine, grad_in.reshape(D, 2, FF), grad_out
```

```python
import functools

import jax
import jax.numpy as jnp
from jax import lax
from jax.experimental import pallas as pl
from jax.experimental.pallas import tpu as pltpu
from jax.sharding import PartitionSpec as P

CAP = 432


def silu_pair(pre):
    sigma = jax.nn.sigmoid(pre)
    return (pre * sigma, sigma * (1.0 + pre * (1.0 - sigma)))


def contract_rows(left, right):
    return lax.dot_general(
        left, right, (((0,), (0,)), ((), ())), preferred_element_type=jnp.float32
    )


def contract_cols(left, right):
    return lax.dot_general(
        left, right, (((1,), (1,)), ((), ())), preferred_element_type=jnp.float32
    )


def swap(value, bit):
    count = lax.axis_size("tok")
    return lax.ppermute(value, "tok", [(k, k ^ bit) for k in range(count)])


def after(value, *others):
    return lax.optimization_barrier((value, *others))[0]


def tok_gather(own, bits):
    held = {0: own}
    for bit in bits:
        held.update({j | bit: swap(held[j], bit) for j in list(held)})
    return [held[j] for j in range(lax.axis_size("tok"))]


def shift(value, lines, share, by, low, high):
    pairs = [
        (q * share + c, (q + by) * share + c)
        for q in range(lines)
        for c in range(share)
        if low <= q <= high and 0 <= q + by < lines
    ]
    return lax.ppermute(value, "hid", pairs)


def turn(value, lines, share, by):
    pairs = [(q * share + c, q * share + (c + by) % share) for q in range(lines) for c in range(share)]
    return lax.ppermute(value, "hid", pairs)


SUBS = 3
MESH = pl.DeviceIdType.MESH


def flip(index, bit):
    return index + bit - 2 * bit * ((index // bit) % 2)


def differ(left, right, bits):
    total = 0
    for bit in bits:
        total = total + bit * (((left // bit) + (right // bit)) % 2)
    return total


def forward_kernel(
    n, share,
    in_hbm, cot_hbm, router_ref, gu_hbm, down_hbm,
    rows_in_hbm, rows_cot_hbm, pre_ref, logit_ref,
    rows, weights, sent, got, logit_sent, logit_got,
    source_sem, own_sem, mate_sem, pass_sem, weight_sem, sent_sem, got_sem,
    logit_sent_sem, logit_got_sem, out_sem,
):
    row = lax.axis_index("tok")
    hid = lax.axis_index("hid")
    place = hid // share
    core = hid % share
    slots, cols = in_hbm.shape
    hidden = weights.shape[2]
    half = hidden // 2
    wide = min(256, half)
    part = slots // SUBS
    ups = [1 << b for b in range((n - 1).bit_length())]
    orders = (ups, ups[::-1])
    sources = (in_hbm, cot_hbm)
    outs = (rows_in_hbm, rows_cot_hbm)
    first_slot = differ(row, place, ups)

    def span(s):
        return pl.ds(s * part, part)

    def remote(src, dst, send, recv, tok, where):
        return pltpu.make_async_remote_copy(
            src_ref=src, dst_ref=dst, send_sem=send, recv_sem=recv,
            device_id=(tok, where), device_id_type=MESH,
        )

    def source_copy(a, s):
        return remote(
            sources[a].at[span(s)], rows.at[a, core, first_slot, span(s)],
            source_sem.at[a, s], own_sem.at[a, first_slot * SUBS + s],
            place, place * share + core,
        )

    def local_copy(a, s):
        return pltpu.make_async_copy(
            sources[a].at[span(s)], rows.at[a, core, 0, span(s)], own_sem.at[a, s]
        )

    def start_sources(a):
        @pl.when(row != place)
        def _():
            for s in range(SUBS):
                source_copy(a, s).start()

        @pl.when(row == place)
        def _():
            for s in range(SUBS):
                local_copy(a, s).start()

    def pass_copy(a, j, s, way):
        index = j * SUBS + s
        piece = rows.at[a, core, j, span(s)]
        if way < 2:
            where = (place + (1 if way else -1)) * share + core
            recv = own_sem.at[a, index]
        else:
            where = place * share + (core + way - 1) % share
            recv = mate_sem.at[a, way - 2, index]
        return remote(piece, piece, pass_sem.at[way, a, index], recv, row, where)

    to_left = jnp.logical_and(place <= row, place > 0)
    to_right = jnp.logical_and(place >= row, place < n - 1)

    def passes(a, j, s, act):
        @pl.when(to_left)
        def _():
            act(pass_copy(a, j, s, 0))

        @pl.when(to_right)
        def _():
            act(pass_copy(a, j, s, 1))

        for by in range(1, share):
            act(pass_copy(a, j, s, by + 1))

    def chain(a, j):
        for s in range(SUBS):
            pltpu.make_async_copy(
                sources[a].at[span(s)], rows.at[a, core, j, span(s)], own_sem.at[a, j * SUBS + s]
            ).wait()
            passes(a, j, s, lambda copy: copy.start())

    def mates(a, j):
        for by in range(1, share):
            other = (core + share - by) % share
            for s in range(SUBS):
                pltpu.make_async_copy(
                    sources[a].at[span(s)],
                    rows.at[a, other, j, span(s)],
                    mate_sem.at[a, by - 1, j * SUBS + s],
                ).wait()

    def product(m, a, j, start):
        total = None
        for c in range(share):
            term = jnp.dot(
                rows[a, c, j],
                weights[m, pl.ds(c * cols, cols), pl.ds(start, wide)],
                preferred_element_type=jnp.float32,
            )
            total = term if total is None else total + term
        return total

    def stage_of(j, bits):
        return [s for s, bit in enumerate(bits) if j & bit][0]

    def message(m, side, j):
        bit = orders[side][stage_of(j, orders[side])]
        i = m * 2 + side
        return remote(
            sent.at[i, j - 1], got.at[i, j - 1],
            sent_sem.at[i, j - 1], got_sem.at[i, j - 1], flip(row, bit), hid,
        )

    def arrivals(j, bits):
        stages = bits if j == 0 else bits[: stage_of(j, bits)]
        return [j ^ bit for bit in stages]

    def block(m, a, side, j):
        i = m * 2 + side
        came = arrivals(j, orders[side])
        for k in came:
            message(m, side, k).wait_recv()

        @pl.loop(0, half // wide)
        def _(step):
            at = pl.multiple_of(step * wide, wide)
            value = product(m, a, j, pl.multiple_of(side * half + at, wide))
            for k in came:
                value = value + got[i, k - 1, :, pl.ds(at, wide)].astype(jnp.float32)
            if j:
                sent[i, j - 1, :, pl.ds(at, wide)] = value.astype(jnp.bfloat16)
            else:
                pre_ref[m, :, pl.ds(pl.multiple_of(side * half + at, wide), wide)] = value

        if j:
            message(m, side, j).start()

    def logit_message(j):
        return remote(
            logit_sent.at[j - 1], logit_got.at[j - 1],
            logit_sent_sem.at[j - 1], logit_got_sem.at[j - 1], flip(row, ups[stage_of(j, ups)]), hid,
        )

    def logit_block(j):
        value = None
        for c in range(share):
            term = contract_cols(router_ref[:, c * cols : (c + 1) * cols], rows[0, c, j])
            value = term if value is None else value + term
        for k in arrivals(j, ups):
            logit_message(k).wait_recv()
            value = value + logit_got[k - 1]
        if j:
            logit_sent[j - 1] = value
            logit_message(j).start()
        else:
            logit_ref[...] = value

    def by_stage(stage, side):
        return [j for j in range(1, n) if stage_of(j, orders[side]) == stage]

    def pair(j, side):
        @pl.loop(0, 2)
        def _(m):
            block(m, 0, side, j)

    loads = [
        pltpu.make_async_copy(gu_hbm, weights.at[pl.ds(0, 2)], weight_sem.at[0]),
        pltpu.make_async_copy(down_hbm, weights.at[2], weight_sem.at[1]),
    ]
    start_sources(0)
    loads[0].start()
    for j in range(n):
        chain(0, j)
        mates(0, j)
        if j == 1:
            start_sources(1)
            loads[0].wait()
            loads[1].start()
        for side in range(2):
            if j and stage_of(j, orders[side]) == 0:
                pair(j, side)
        if j and stage_of(j, ups) == 0:
            logit_block(j)
    out_in = pltpu.make_async_copy(rows.at[0], rows_in_hbm, out_sem.at[0])
    out_in.start()
    chain(1, 0)
    chain(1, 1)
    for stage in range(1, len(ups)):
        for j in by_stage(stage, 0):
            logit_block(j)
        for m in range(2):
            for side in range(2):
                for j in by_stage(stage, side):
                    block(m, 0, side, j)
            if stage == 1:
                if m == 0:
                    chain(1, 2)
    loads[1].wait()
    for j in range(n):
        if j > 2:
            chain(1, j)
        mates(1, j)
        for side in range(2):
            if j and stage_of(j, orders[side]) == 0:
                block(2, 1, side, j)
    out_cot = pltpu.make_async_copy(rows.at[1], rows_cot_hbm, out_sem.at[1])
    out_cot.start()
    pair(0, 0)
    pair(0, 1)
    logit_block(0)
    for stage in range(1, len(ups)):
        for side in range(2):
            for j in by_stage(stage, side):
                block(2, 1, side, j)
    for side in range(2):
        block(2, 1, side, 0)

    out_in.wait()
    out_cot.wait()
    for a in range(2):
        @pl.when(row != place)
        def _():
            for s in range(SUBS):
                source_copy(a, s).wait_send()

        for j in range(n):
            for s in range(SUBS):
                passes(a, j, s, lambda copy: copy.wait_send())
    for j in range(1, n):
        logit_message(j).wait_send()
        for side in range(2):
            for m in range(3):
                message(m, side, j).wait_send()


def forward_call(n, share, picked_in, picked_cot, router_cols, gate_up, down):
    slots, cols = picked_in.shape
    depth, hidden = down.shape
    experts = router_cols.shape[0]
    half = hidden // 2
    hbm = pl.BlockSpec(memory_space=pltpu.HBM)
    vmem = pl.BlockSpec(memory_space=pltpu.VMEM)
    spread = (share, n, slots, cols)
    dma = pltpu.SemaphoreType.DMA
    return pl.pallas_call(
        functools.partial(forward_kernel, n, share),
        in_specs=[hbm, hbm, vmem, hbm, hbm],
        out_specs=[hbm, hbm, vmem, vmem],
        out_shape=[
            jax.ShapeDtypeStruct(spread, jnp.bfloat16),
            jax.ShapeDtypeStruct(spread, jnp.bfloat16),
            jax.ShapeDtypeStruct((3, slots, hidden), jnp.float32),
            jax.ShapeDtypeStruct((experts, slots), jnp.float32),
        ],
        scratch_shapes=[
            pltpu.VMEM((2, *spread), jnp.bfloat16),
            pltpu.VMEM((3, depth, hidden), jnp.bfloat16),
            pltpu.VMEM((6, n - 1, slots, half), jnp.bfloat16),
            pltpu.VMEM((6, n - 1, slots, half), jnp.bfloat16),
            pltpu.VMEM((n - 1, experts, slots), jnp.float32),
            pltpu.VMEM((n - 1, experts, slots), jnp.float32),
            dma((2, SUBS)),
            dma((2, n * SUBS)),
            dma((2, share - 1, n * SUBS)),
            dma((share + 1, 2, n * SUBS)),
            dma((2,)),
            dma((6, n - 1)),
            dma((6, n - 1)),
            dma((n - 1,)),
            dma((n - 1,)),
            dma((2,)),
        ],
        compiler_params=pltpu.CompilerParams(vmem_limit_bytes=60 * 2**20, has_side_effects=True),
        cost_estimate=pl.CostEstimate(
            flops=6 * n * slots * depth * hidden, bytes_accessed=60 * 2**20, transcendentals=0
        ),
        name="forward",
    )(picked_in, picked_cot, router_cols, gate_up, down)


def grad_dot(rows_ref, refs):
    total = None
    for j, ref in enumerate(refs):
        term = contract_rows(rows_ref[0, j], ref[...])
        total = term if total is None else total + term
    return total


def pair_body(*refs):
    count = (len(refs) - 2) // 2
    rows_ref, out_ref = refs[0], refs[-1]
    out_ref[:, 0, :] = grad_dot(rows_ref, refs[1 : 1 + count])
    out_ref[:, 1, :] = grad_dot(rows_ref, refs[1 + count : -1])


def single_body(*refs):
    refs[-1][...] = grad_dot(refs[0], refs[1:-1])


def grad_call(body, rows, grads, middle, name):
    share, count, slots, cols = rows.shape
    hidden = grads[0].shape[1]
    tile = 256 if cols % 256 == 0 else 128
    per = cols // tile
    whole = [pl.BlockSpec((slots, hidden), lambda i: (0, 0)) for _ in grads]
    return pl.pallas_call(
        body,
        grid=(share * per,),
        in_specs=[pl.BlockSpec((1, count, slots, tile), lambda i: (i // per, 0, 0, i % per))] + whole,
        out_specs=pl.BlockSpec((tile, *middle, hidden), lambda i: (i,) + (0,) * (len(middle) + 1)),
        out_shape=jax.ShapeDtypeStruct((share * cols, *middle, hidden), jnp.float32),
        compiler_params=pltpu.CompilerParams(vmem_limit_bytes=40 * 2**20),
        cost_estimate=pl.CostEstimate(
            flops=2 * share * cols * slots * hidden * len(grads),
            bytes_accessed=rows.size * 2 + share * cols * hidden * 4 * max(1, *middle, 1),
            transcendentals=0,
        ),
        name=name,
    )(rows, *grads)


def local(tokens, cotangent, expert_choice, router, gate_up, w_down):
    n_tok = lax.axis_size("tok")
    n_hid = lax.axis_size("hid")
    share = n_hid // n_tok
    local_cols = tokens.shape[1]
    weight_rows, hidden_local = w_down.shape
    half = hidden_local // 2
    ups = [1 << b for b in range((n_tok - 1).bit_length())]
    downs = ups[::-1]
    row = lax.axis_index("tok")
    place = lax.axis_index("hid") // share
    core = lax.axis_index("hid") % share
    first = expert_choice[:, 0]
    second = expert_choice[:, 1]
    in_first = first == 0
    in_second = second == 0
    routed = jnp.logical_or(in_first, in_second)
    flags = routed.astype(jnp.int32)
    slot_rank = jnp.cumsum(flags) - flags
    slot_ids = jnp.arange(CAP, dtype=jnp.int32)
    placed = jnp.logical_and(routed[None, :], slot_rank[None, :] == slot_ids[:, None])
    one_hot = placed.astype(jnp.bfloat16)
    forth = [
        (k * n_hid + t * share + c, t * n_hid + (k ^ t) * share + c)
        for k in range(n_tok)
        for t in range(n_tok)
        for c in range(share)
    ]
    back_pairs = [(b, a) for a, b in forth]

    def pick(values):
        return jnp.dot(one_hot, values, preferred_element_type=jnp.float32).astype(jnp.bfloat16)

    router_cols = lax.dynamic_slice_in_dim(router, row * weight_rows, weight_rows, 1)
    weights = lax.optimization_barrier(jnp.transpose(gate_up, (1, 0, 2)))
    w_gate, w_up = weights[0], weights[1]
    pieces_in, pieces_cot, pre, logits = forward_call(
        n_tok, share, pick(tokens), pick(cotangent), router_cols, weights, w_down
    )
    gate_pre, up_pre, raw = pre[0], pre[1], pre[2]
    slot_other = jnp.sum(jnp.where(placed, (first + second)[None, :], 0), axis=1)
    filled = jnp.any(placed, axis=1)
    labels = jnp.arange(logits.shape[0], dtype=jnp.int32)
    other_logit = jnp.sum(jnp.where(slot_other[None, :] == labels[:, None], logits, 0.0), axis=0)
    slot_gate = jnp.where(filled, jax.nn.sigmoid(logits[0] - other_logit), 0.0)

    active, slope = silu_pair(gate_pre)
    product = active * up_pre
    scale = slot_gate[:, None]
    scaled = (scale * product).astype(jnp.bfloat16)
    scores = jnp.sum(product * raw, axis=1)
    upstream = scale * raw
    own_gate = (upstream * up_pre * slope).astype(jnp.bfloat16)
    grad_gate = tok_gather(own_gate, ups)
    grad_up = tok_gather((upstream * active).astype(jnp.bfloat16), downs)
    bit = 1
    while bit < n_hid:
        scores = scores + lax.ppermute(scores, "hid", [(h, h ^ bit) for h in range(n_hid)])
        bit *= 2
    scaled_left = tok_gather(after(scaled[:, :half], grad_gate[1]), ups)
    scaled_right = tok_gather(after(scaled[:, half:], grad_up[n_tok // 2]), downs)

    backs = [
        contract_cols(grad_gate[j], w_gate) + contract_cols(grad_up[j], w_up) for j in range(n_tok)
    ]
    parts = [jnp.stack([b[:, c * local_cols : (c + 1) * local_cols].astype(jnp.bfloat16) for b in backs]) for c in range(share)]

    def of_core(c):
        chosen = parts[0]
        for other in range(1, share):
            chosen = jnp.where(c % share == other, parts[other], chosen)
        return chosen

    held = of_core(core).astype(jnp.float32)
    for by in range(1, share):
        held = held + turn(of_core(core + by), n_tok, share, by).astype(jnp.float32)

    def chunk(index):
        return lax.dynamic_index_in_dim(held, jnp.clip(index, 0, n_tok - 1), 0, keepdims=False)

    from_left = jnp.zeros(held.shape[1:], jnp.float32)
    from_right = from_left
    for step in range(1, n_tok):
        go_right = chunk(place + n_tok - step) + from_left
        go_left = chunk(place - n_tok + step) + from_right
        from_left = shift(go_right.astype(jnp.bfloat16), n_tok, share, 1, 0, step - 1).astype(jnp.float32)
        from_right = shift(go_left.astype(jnp.bfloat16), n_tok, share, -1, n_tok - step, n_tok).astype(jnp.float32)
    reduced = (chunk(place) + from_left + from_right).astype(jnp.bfloat16)

    d_gate_up = grad_call(pair_body, pieces_in, grad_gate + grad_up, (2,), "pair_grad")
    d_down = grad_call(single_body, pieces_cot, [jnp.concatenate([a, b], axis=1) for a, b in zip(scaled_left, scaled_right)], (), "down_grad")
    back_cols = lax.ppermute(reduced, ("tok", "hid"), back_pairs)
    grad_tokens = contract_rows(one_hot, back_cols).astype(jnp.bfloat16)
    token_score = jnp.sum(jnp.where(placed, scores[:, None], 0.0), axis=0)
    d_combine = jnp.stack(
        [jnp.where(in_first, token_score, 0.0), jnp.where(in_second, token_score, 0.0)], axis=1
    )
    return (grad_tokens, d_combine, d_gate_up, d_down)


def solution(mesh):
    in_specs = (
        P("tok", "hid"),
        P("tok", "hid"),
        P("tok", None),
        P(),
        P("tok", None, "hid"),
        P("tok", "hid"),
    )
    out_specs = (P("tok", "hid"), P("tok", None), P("tok", None, "hid"), P("tok", "hid"))
    return jax.shard_map(local, mesh=mesh, in_specs=in_specs, out_specs=out_specs, check_vma=False)
```

```python
import functools

import jax
import jax.numpy as jnp
from jax import lax
from jax.experimental import pallas as pl
from jax.experimental.pallas import tpu as pltpu
from jax.sharding import PartitionSpec as P

CAP = 432


def silu_pair(pre):
    sigma = jax.nn.sigmoid(pre)
    return (pre * sigma, sigma * (1.0 + pre * (1.0 - sigma)))


def contract_rows(left, right):
    return lax.dot_general(
        left, right, (((0,), (0,)), ((), ())), preferred_element_type=jnp.float32
    )


def contract_cols(left, right):
    return lax.dot_general(
        left, right, (((1,), (1,)), ((), ())), preferred_element_type=jnp.float32
    )


SUBS = 3
MESH = pl.DeviceIdType.MESH


def flip(index, bit):
    return index + bit - 2 * bit * ((index // bit) % 2)


def differ(left, right, bits):
    total = 0
    for bit in bits:
        total = total + bit * (((left // bit) + (right // bit)) % 2)
    return total


def forward_kernel(
    n, share,
    in_hbm, cot_hbm, router_ref, gu_hbm, down_hbm,
    rows_in_hbm, rows_cot_hbm, pre_ref, logit_ref,
    rows, weights, sent, got, logit_sent, logit_got,
    source_sem, own_sem, mate_sem, pass_sem, weight_sem, sent_sem, got_sem,
    logit_sent_sem, logit_got_sem, out_sem,
):
    row = lax.axis_index("tok")
    hid = lax.axis_index("hid")
    place = hid // share
    core = hid % share
    slots, cols = in_hbm.shape
    hidden = weights.shape[2]
    half = hidden // 2
    wide = min(256, half)
    part = slots // SUBS
    ups = [1 << b for b in range((n - 1).bit_length())]
    orders = (ups, ups[::-1])
    sources = (in_hbm, cot_hbm)
    outs = (rows_in_hbm, rows_cot_hbm)
    first_slot = differ(row, place, ups)

    def span(s):
        return pl.ds(s * part, part)

    def remote(src, dst, send, recv, tok, where):
        return pltpu.make_async_remote_copy(
            src_ref=src, dst_ref=dst, send_sem=send, recv_sem=recv,
            device_id=(tok, where), device_id_type=MESH,
        )

    def source_copy(a, s):
        return remote(
            sources[a].at[span(s)], rows.at[a, core, first_slot, span(s)],
            source_sem.at[a, s], own_sem.at[a, first_slot * SUBS + s],
            place, place * share + core,
        )

    def local_copy(a, s):
        return pltpu.make_async_copy(
            sources[a].at[span(s)], rows.at[a, core, 0, span(s)], own_sem.at[a, s]
        )

    def start_sources(a):
        @pl.when(row != place)
        def _():
            for s in range(SUBS):
                source_copy(a, s).start()

        @pl.when(row == place)
        def _():
            for s in range(SUBS):
                local_copy(a, s).start()

    def pass_copy(a, j, s, way):
        index = j * SUBS + s
        piece = rows.at[a, core, j, span(s)]
        if way < 2:
            where = (place + (1 if way else -1)) * share + core
            recv = own_sem.at[a, index]
        else:
            where = place * share + (core + way - 1) % share
            recv = mate_sem.at[a, way - 2, index]
        return remote(piece, piece, pass_sem.at[way, a, index], recv, row, where)

    to_left = jnp.logical_and(place <= row, place > 0)
    to_right = jnp.logical_and(place >= row, place < n - 1)

    def passes(a, j, s, act):
        @pl.when(to_left)
        def _():
            act(pass_copy(a, j, s, 0))

        @pl.when(to_right)
        def _():
            act(pass_copy(a, j, s, 1))

        for by in range(1, share):
            act(pass_copy(a, j, s, by + 1))

    def chain(a, j):
        for s in range(SUBS):
            pltpu.make_async_copy(
                sources[a].at[span(s)], rows.at[a, core, j, span(s)], own_sem.at[a, j * SUBS + s]
            ).wait()
            passes(a, j, s, lambda copy: copy.start())

    def mates(a, j):
        for by in range(1, share):
            other = (core + share - by) % share
            for s in range(SUBS):
                pltpu.make_async_copy(
                    sources[a].at[span(s)],
                    rows.at[a, other, j, span(s)],
                    mate_sem.at[a, by - 1, j * SUBS + s],
                ).wait()

    def product(m, a, j, start):
        total = None
        for c in range(share):
            term = jnp.dot(
                rows[a, c, j],
                weights[m, pl.ds(c * cols, cols), pl.ds(start, wide)],
                preferred_element_type=jnp.float32,
            )
            total = term if total is None else total + term
        return total

    def stage_of(j, bits):
        return [s for s, bit in enumerate(bits) if j & bit][0]

    def message(m, side, j):
        bit = orders[side][stage_of(j, orders[side])]
        i = m * 2 + side
        return remote(
            sent.at[i, j - 1], got.at[i, j - 1],
            sent_sem.at[i, j - 1], got_sem.at[i, j - 1], flip(row, bit), hid,
        )

    def arrivals(j, bits):
        stages = bits if j == 0 else bits[: stage_of(j, bits)]
        return [j ^ bit for bit in stages]

    def block(m, a, side, j):
        i = m * 2 + side
        came = arrivals(j, orders[side])
        for k in came:
            message(m, side, k).wait_recv()

        @pl.loop(0, half // wide)
        def _(step):
            at = pl.multiple_of(step * wide, wide)
            value = product(m, a, j, pl.multiple_of(side * half + at, wide))
            for k in came:
                value = value + got[i, k - 1, :, pl.ds(at, wide)].astype(jnp.float32)
            if j:
                sent[i, j - 1, :, pl.ds(at, wide)] = value.astype(jnp.bfloat16)
            else:
                pre_ref[m, :, pl.ds(pl.multiple_of(side * half + at, wide), wide)] = value

        if j:
            message(m, side, j).start()

    def logit_message(j):
        return remote(
            logit_sent.at[j - 1], logit_got.at[j - 1],
            logit_sent_sem.at[j - 1], logit_got_sem.at[j - 1], flip(row, ups[stage_of(j, ups)]), hid,
        )

    def logit_block(j):
        value = None
        for c in range(share):
            term = contract_cols(router_ref[:, c * cols : (c + 1) * cols], rows[0, c, j])
            value = term if value is None else value + term
        for k in arrivals(j, ups):
            logit_message(k).wait_recv()
            value = value + logit_got[k - 1]
        if j:
            logit_sent[j - 1] = value
            logit_message(j).start()
        else:
            logit_ref[...] = value

    def by_stage(stage, side):
        return [j for j in range(1, n) if stage_of(j, orders[side]) == stage]

    def pair(j, side):
        @pl.loop(0, 2)
        def _(m):
            block(m, 0, side, j)

    loads = [
        pltpu.make_async_copy(gu_hbm, weights.at[pl.ds(0, 2)], weight_sem.at[0]),
        pltpu.make_async_copy(down_hbm, weights.at[2], weight_sem.at[1]),
    ]
    start_sources(0)
    loads[0].start()
    for j in range(n):
        chain(0, j)
        mates(0, j)
        if j == 1:
            start_sources(1)
            loads[0].wait()
            loads[1].start()
        for side in range(2):
            if j and stage_of(j, orders[side]) == 0:
                pair(j, side)
        if j and stage_of(j, ups) == 0:
            logit_block(j)
    out_in = pltpu.make_async_copy(rows.at[0], rows_in_hbm, out_sem.at[0])
    out_in.start()
    chain(1, 0)
    chain(1, 1)
    for stage in range(1, len(ups)):
        for j in by_stage(stage, 0):
            logit_block(j)
        for m in range(2):
            for side in range(2):
                for j in by_stage(stage, side):
                    block(m, 0, side, j)
            if stage == 1:
                if m == 0:
                    chain(1, 2)
    loads[1].wait()
    for j in range(n):
        if j > 2:
            chain(1, j)
        mates(1, j)
        for side in range(2):
            if j and stage_of(j, orders[side]) == 0:
                block(2, 1, side, j)
    out_cot = pltpu.make_async_copy(rows.at[1], rows_cot_hbm, out_sem.at[1])
    out_cot.start()
    pair(0, 0)
    pair(0, 1)
    logit_block(0)
    for stage in range(1, len(ups)):
        for side in range(2):
            for j in by_stage(stage, side):
                block(2, 1, side, j)
    for side in range(2):
        block(2, 1, side, 0)

    out_in.wait()
    out_cot.wait()
    for a in range(2):
        @pl.when(row != place)
        def _():
            for s in range(SUBS):
                source_copy(a, s).wait_send()

        for j in range(n):
            for s in range(SUBS):
                passes(a, j, s, lambda copy: copy.wait_send())
    for j in range(1, n):
        logit_message(j).wait_send()
        for side in range(2):
            for m in range(3):
                message(m, side, j).wait_send()


def forward_call(n, share, picked_in, picked_cot, router_cols, gate_up, down):
    slots, cols = picked_in.shape
    depth, hidden = down.shape
    experts = router_cols.shape[0]
    half = hidden // 2
    hbm = pl.BlockSpec(memory_space=pltpu.HBM)
    vmem = pl.BlockSpec(memory_space=pltpu.VMEM)
    spread = (share, n, slots, cols)
    dma = pltpu.SemaphoreType.DMA
    return pl.pallas_call(
        functools.partial(forward_kernel, n, share),
        in_specs=[hbm, hbm, vmem, hbm, hbm],
        out_specs=[hbm, hbm, vmem, vmem],
        out_shape=[
            jax.ShapeDtypeStruct(spread, jnp.bfloat16),
            jax.ShapeDtypeStruct(spread, jnp.bfloat16),
            jax.ShapeDtypeStruct((3, slots, hidden), jnp.float32),
            jax.ShapeDtypeStruct((experts, slots), jnp.float32),
        ],
        scratch_shapes=[
            pltpu.VMEM((2, *spread), jnp.bfloat16),
            pltpu.VMEM((3, depth, hidden), jnp.bfloat16),
            pltpu.VMEM((6, n - 1, slots, half), jnp.bfloat16),
            pltpu.VMEM((6, n - 1, slots, half), jnp.bfloat16),
            pltpu.VMEM((n - 1, experts, slots), jnp.float32),
            pltpu.VMEM((n - 1, experts, slots), jnp.float32),
            dma((2, SUBS)),
            dma((2, n * SUBS)),
            dma((2, share - 1, n * SUBS)),
            dma((share + 1, 2, n * SUBS)),
            dma((2,)),
            dma((6, n - 1)),
            dma((6, n - 1)),
            dma((n - 1,)),
            dma((n - 1,)),
            dma((2,)),
        ],
        compiler_params=pltpu.CompilerParams(vmem_limit_bytes=60 * 2**20, has_side_effects=True),
        cost_estimate=pl.CostEstimate(
            flops=6 * n * slots * depth * hidden, bytes_accessed=60 * 2**20, transcendentals=0
        ),
        name="forward",
    )(picked_in, picked_cot, router_cols, gate_up, down)


def backward_kernel(
    n, share, tile,
    grads_hbm, score_ref, weights_hbm, rows_in_hbm, rows_cot_hbm,
    back_ref, score_out_ref, pair_hbm, down_hbm,
    grads, weights, rows, kept, mate_sent, mate_got, flow_got, flow_sent, flow_sum, last_got,
    pair_tile, down_tile, score_got,
    load_sem, grad_sent_sem, grad_got_sem, mate_sent_sem, mate_got_sem, flow_sent_sem, flow_got_sem,
    last_sem, tile_sem, score_sent_sem, score_got_sem,
):
    row = lax.axis_index("tok")
    hid = lax.axis_index("hid")
    n_hid = n * share
    place = hid // share
    core = hid % share
    slots, hidden = grads.shape[2:]
    cols = rows.shape[4]
    half = hidden // 2
    part = slots // SUBS
    per = cols // tile
    bits = [1 << b for b in range((n - 1).bit_length())]
    singles = [j for j in range(1, n) if j in bits]
    others = sorted((j for j in range(1, n) if j not in bits), key=lambda j: bin(j).count("1"))

    def remote(src, dst, send, recv, tok, where):
        return pltpu.make_async_remote_copy(
            src_ref=src, dst_ref=dst, send_sem=send, recv_sem=recv,
            device_id=(tok, where), device_id_type=MESH,
        )

    def route(j, side):
        through = [bit for bit in bits if j & bit]
        return through[-1] if side else through[0]

    def grad_message(x, j, side):
        bit = route(j, side)
        columns = pl.ds(side * half, half)
        return remote(
            grads.at[x, j ^ bit, :, columns], grads.at[x, j, :, columns],
            grad_sent_sem.at[x, j - 1, side], grad_got_sem.at[x, j - 1, side], flip(row, bit), hid,
        )

    def direct(x):
        for j in singles:
            for side in range(2):
                grad_message(x, j, side).start()

    def onward(x, source):
        for j in others:
            for side in range(2):
                if j ^ route(j, side) == source:
                    grad_message(x, j, side).start()

    def take(x, j):
        for side in range(2):
            grad_message(x, j, side).wait_recv()
        onward(x, j)

    def mate_copy(j, by):
        return remote(
            mate_sent.at[by - 1, j], mate_got.at[by - 1, j],
            mate_sent_sem.at[by - 1, j], mate_got_sem.at[by - 1, j],
            row, place * share + (core + by) % share,
        )

    def back_tile(j, start):
        total = None
        for x in range(2):
            term = contract_cols(grads[x, j], weights[x, pl.ds(start, tile), :])
            total = term if total is None else total + term
        return total

    def back(j):
        for by in range(share - 1, -1, -1):
            base = (core + by) % share * cols

            @pl.loop(0, per)
            def _(step):
                at = pl.multiple_of(step * tile, tile)
                value = back_tile(j, pl.multiple_of(base + at, tile))
                if by:
                    mate_sent[by - 1, j, :, pl.ds(at, tile)] = value.astype(jnp.bfloat16)
                else:
                    kept[j, :, pl.ds(at, tile)] = value

            if by:
                mate_copy(j, by).start()

    from_left = jnp.logical_and(place <= row, place > 0)
    from_right = jnp.logical_and(place >= row, place < n - 1)

    def span(s):
        return pl.ds(pl.multiple_of(s * part, part), part)

    def flow_copy(j, s, way):
        return remote(
            flow_sent.at[j, span(s)], flow_got.at[way, j, span(s)],
            flow_sent_sem.at[j, s], flow_got_sem.at[way, j, s],
            row, (place + (-1 if way else 1)) * share + core,
        )

    def last_copy(j, s):
        tok = row
        for bit in bits:
            if j & bit:
                tok = flip(tok, bit)
        return remote(
            flow_sent.at[j, span(s)], last_got.at[span(s)],
            flow_sent_sem.at[j, s], last_sem.at[s], tok, hid,
        )

    def flow_moves(j, s, act):
        @pl.when(place < row)
        def _():
            act(flow_copy(j, s, 0))

        @pl.when(place > row)
        def _():
            act(flow_copy(j, s, 1))

        if j:
            @pl.when(place == row)
            def _():
                act(last_copy(j, s))

    def flow(j, s):
        value = kept[j, span(s)]
        for by in range(1, share):
            value = value + mate_got[by - 1, j, span(s)].astype(jnp.float32)
        flow_sum[...] = value
        for way, present in enumerate((from_left, from_right)):
            @pl.when(present)
            def _():
                flow_copy(j, s, way).wait_recv()
                flow_sum[...] += flow_got[way, j, span(s)].astype(jnp.float32)

        flow_sent[j, span(s)] = flow_sum[...].astype(jnp.bfloat16)
        if j == 0:
            @pl.when(place == row)
            def _():
                back_ref[span(s)] = flow_sum[...].astype(jnp.bfloat16)

        flow_moves(j, s, lambda copy: copy.start())

    def mates(j):
        for by in range(1, share):
            mate_copy(j, by).wait_recv()

    def flows(j):
        mates(j)

        @pl.loop(0, SUBS)
        def _(s):
            flow(j, s)

    def tile_copy(x, i):
        slot = i % 2
        at = pl.ds(pl.multiple_of(i * tile, tile), tile)
        if x:
            return pltpu.make_async_copy(down_tile.at[slot], down_hbm.at[at], tile_sem.at[1, slot])
        return pltpu.make_async_copy(pair_tile.at[slot], pair_hbm.at[at], tile_sem.at[0, slot])

    def tile_sum(a, x, i):
        at = pl.ds(pl.multiple_of(i % per * tile, tile), tile)
        total = None
        for j in range(n):
            term = contract_rows(rows[a, i // per, j, :, at], grads[x, j])
            total = term if total is None else total + term
        return total

    def pair_step(i):
        @pl.when(i >= 2)
        def _():
            tile_copy(0, i - 2).wait()

        for x in range(2):
            pair_tile[i % 2, :, x, :] = tile_sum(0, x, i)
        tile_copy(0, i).start()

    def down_step(i):
        @pl.when(i >= 2)
        def _():
            tile_copy(1, i - 2).wait()

        down_tile[i % 2] = tile_sum(1, 2, i)
        tile_copy(1, i).start()

    def score_copy(by):
        return remote(
            score_ref, score_got.at[by - 1],
            score_sent_sem.at[by - 1], score_got_sem.at[by - 1], row, (hid + by) % n_hid,
        )

    own_loads = [pltpu.make_async_copy(grads_hbm.at[x], grads.at[x, 0], load_sem.at[x]) for x in range(3)]
    weight_load = pltpu.make_async_copy(weights_hbm, weights, load_sem.at[3])
    row_loads = [
        pltpu.make_async_copy(rows_in_hbm, rows.at[0], load_sem.at[4]),
        pltpu.make_async_copy(rows_cot_hbm, rows.at[1], load_sem.at[5]),
    ]
    for load in own_loads:
        load.start()
    weight_load.start()
    for x in range(2):
        own_loads[x].wait()
        direct(x)
    for by in range(1, n_hid):
        score_copy(by).start()
    weight_load.wait()
    for load in row_loads:
        load.start()
    back(0)
    flows(0)
    own_loads[2].wait()
    for x in range(2):
        for j in singles:
            take(x, j)
    direct(2)
    for j in singles:
        back(j)
        flows(j)
    for j in others[:-1]:
        for x in range(2):
            take(x, j)
        back(j)
        flows(j)
    end = others[-1]
    for x in range(2):
        take(x, end)
    back(end)
    mates(end)
    for load in row_loads:
        load.wait()
    tiles = share * per
    each = -(-tiles // SUBS)

    @pl.loop(0, SUBS)
    def _(s):
        @pl.loop(0, each)
        def _(step):
            @pl.when(s * each + step < tiles)
            def _():
                pair_step(s * each + step)

        flow(end, s)

    for j in singles + others:
        take(2, j)

    @pl.loop(0, tiles)
    def _(i):
        down_step(i)

    total = score_ref[...]
    for by in range(1, n_hid):
        score_copy(by).wait_recv()
        total = total + score_got[by - 1]
    score_out_ref[...] = total

    @pl.when(place != row)
    def _():
        for s in range(SUBS):
            last_copy(1, s).wait_recv()
        back_ref[...] = last_got[...]

    for i in range(max(0, tiles - 2), tiles):
        for x in range(2):
            tile_copy(x, i).wait()
    for by in range(1, n_hid):
        score_copy(by).wait_send()
    for x in range(3):
        for j in range(1, n):
            for side in range(2):
                grad_message(x, j, side).wait_send()
    for j in range(n):
        for by in range(1, share):
            mate_copy(j, by).wait_send()
        for s in range(SUBS):
            flow_moves(j, s, lambda copy: copy.wait_send())


def backward_call(n, share, own, scores, weights, rows_in, rows_cot):
    _, slots, hidden = own.shape
    cols = rows_in.shape[3]
    depth = share * cols
    tile = 256 if cols % 256 == 0 else 128
    part = slots // SUBS
    n_hid = n * share
    hbm = pl.BlockSpec(memory_space=pltpu.HBM)
    vmem = pl.BlockSpec(memory_space=pltpu.VMEM)
    dma = pltpu.SemaphoreType.DMA
    half = jnp.bfloat16
    return pl.pallas_call(
        functools.partial(backward_kernel, n, share, tile),
        in_specs=[hbm, vmem, hbm, hbm, hbm],
        out_specs=[vmem, vmem, hbm, hbm],
        out_shape=[
            jax.ShapeDtypeStruct((slots, cols), half),
            jax.ShapeDtypeStruct(scores.shape, jnp.float32),
            jax.ShapeDtypeStruct((depth, 2, hidden), jnp.float32),
            jax.ShapeDtypeStruct((depth, hidden), jnp.float32),
        ],
        scratch_shapes=[
            pltpu.VMEM((3, n, slots, hidden), half),
            pltpu.VMEM((2, depth, hidden), half),
            pltpu.VMEM((2, share, n, slots, cols), half),
            pltpu.VMEM((n, slots, cols), jnp.float32),
            pltpu.VMEM((share - 1, n, slots, cols), half),
            pltpu.VMEM((share - 1, n, slots, cols), half),
            pltpu.VMEM((2, n, slots, cols), half),
            pltpu.VMEM((n, slots, cols), half),
            pltpu.VMEM((part, cols), jnp.float32),
            pltpu.VMEM((slots, cols), half),
            pltpu.VMEM((2, tile, 2, hidden), jnp.float32),
            pltpu.VMEM((2, tile, hidden), jnp.float32),
            pltpu.VMEM((n_hid - 1, *scores.shape), jnp.float32),
            dma((6,)),
            dma((3, n - 1, 2)),
            dma((3, n - 1, 2)),
            dma((share - 1, n)),
            dma((share - 1, n)),
            dma((n, SUBS)),
            dma((2, n, SUBS)),
            dma((SUBS,)),
            dma((2, 2)),
            dma((n_hid - 1,)),
            dma((n_hid - 1,)),
        ],
        compiler_params=pltpu.CompilerParams(vmem_limit_bytes=63 * 2**20, has_side_effects=True),
        cost_estimate=pl.CostEstimate(
            flops=10 * n * slots * depth * hidden, bytes_accessed=60 * 2**20, transcendentals=0
        ),
        name="backward",
    )(own, scores, weights, rows_in, rows_cot)


def local(tokens, cotangent, expert_choice, router, gate_up, w_down):
    n_tok = lax.axis_size("tok")
    n_hid = lax.axis_size("hid")
    share = n_hid // n_tok
    weight_rows = w_down.shape[0]
    row = lax.axis_index("tok")
    first = expert_choice[:, 0]
    second = expert_choice[:, 1]
    in_first = first == 0
    in_second = second == 0
    routed = jnp.logical_or(in_first, in_second)
    flags = routed.astype(jnp.int32)
    slot_rank = jnp.cumsum(flags) - flags
    slot_ids = jnp.arange(CAP, dtype=jnp.int32)
    placed = jnp.logical_and(routed[None, :], slot_rank[None, :] == slot_ids[:, None])
    one_hot = placed.astype(jnp.bfloat16)
    def pick(values):
        return jnp.dot(one_hot, values, preferred_element_type=jnp.float32).astype(jnp.bfloat16)

    router_cols = lax.dynamic_slice_in_dim(router, row * weight_rows, weight_rows, 1)
    weights = lax.optimization_barrier(jnp.transpose(gate_up, (1, 0, 2)))
    pieces_in, pieces_cot, pre, logits = forward_call(
        n_tok, share, pick(tokens), pick(cotangent), router_cols, weights, w_down
    )
    gate_pre, up_pre, raw = pre[0], pre[1], pre[2]
    slot_other = jnp.sum(jnp.where(placed, (first + second)[None, :], 0), axis=1)
    filled = jnp.any(placed, axis=1)
    labels = jnp.arange(logits.shape[0], dtype=jnp.int32)
    other_logit = jnp.sum(jnp.where(slot_other[None, :] == labels[:, None], logits, 0.0), axis=0)
    slot_gate = jnp.where(filled, jax.nn.sigmoid(logits[0] - other_logit), 0.0)

    active, slope = silu_pair(gate_pre)
    product = active * up_pre
    scale = slot_gate[:, None]
    score_part = jnp.sum(product * raw, axis=1)
    upstream = scale * raw
    own = jnp.stack(
        [
            (upstream * up_pre * slope).astype(jnp.bfloat16),
            (upstream * active).astype(jnp.bfloat16),
            (scale * product).astype(jnp.bfloat16),
        ]
    )
    back_cols, scores, d_gate_up, d_down = backward_call(
        n_tok, share, own, score_part[None, :], weights, pieces_in, pieces_cot
    )
    scores = scores[0]
    grad_tokens = contract_rows(one_hot, back_cols).astype(jnp.bfloat16)
    token_score = jnp.sum(jnp.where(placed, scores[:, None], 0.0), axis=0)
    d_combine = jnp.stack(
        [jnp.where(in_first, token_score, 0.0), jnp.where(in_second, token_score, 0.0)], axis=1
    )
    return (grad_tokens, d_combine, d_gate_up, d_down)


def solution(mesh):
    in_specs = (
        P("tok", "hid"),
        P("tok", "hid"),
        P("tok", None),
        P(),
        P("tok", None, "hid"),
        P("tok", "hid"),
    )
    out_specs = (P("tok", "hid"), P("tok", None), P("tok", None, "hid"), P("tok", "hid"))
    return jax.shard_map(local, mesh=mesh, in_specs=in_specs, out_specs=out_specs, check_vma=False)
```

```python
import functools

import jax
import jax.numpy as jnp
from jax import lax
from jax.experimental import pallas as pl
from jax.experimental.pallas import tpu as pltpu
from jax.sharding import PartitionSpec as P

CAP = 432


def silu_pair(pre):
    sigma = jax.nn.sigmoid(pre)
    return (pre * sigma, sigma * (1.0 + pre * (1.0 - sigma)))


def contract_rows(left, right):
    return lax.dot_general(
        left, right, (((0,), (0,)), ((), ())), preferred_element_type=jnp.float32
    )


def contract_cols(left, right):
    return lax.dot_general(
        left, right, (((1,), (1,)), ((), ())), preferred_element_type=jnp.float32
    )


SUBS = 9
MESH = pl.DeviceIdType.MESH


def flip(index, bit):
    return index + bit - 2 * bit * ((index // bit) % 2)


def differ(left, right, bits):
    total = 0
    for bit in bits:
        total = total + bit * (((left // bit) + (right // bit)) % 2)
    return total


def forward_kernel(
    n, share,
    in_hbm, full_hbm, one_hot_ref, router_ref, gu_hbm, down_hbm,
    rows_in_hbm, rows_cot_hbm, cot_hbm, weights_hbm, pre_ref, logit_ref,
    rows, weights, full, picked, strip, sent, got, logit_sent, logit_got,
    source_sem, own_sem, mate_sem, pass_sem, weight_sem, strip_sem, sent_sem, got_sem,
    logit_sent_sem, logit_got_sem, out_sem,
):
    row = lax.axis_index("tok")
    hid = lax.axis_index("hid")
    place = hid // share
    core = hid % share
    slots, cols = in_hbm.shape
    hidden = weights.shape[2]
    half = hidden // 2
    wide = min(256, half)
    wide_pick = 256 if cols % 256 == 0 else 128
    part = slots // SUBS
    ups = [1 << b for b in range((n - 1).bit_length())]
    orders = (ups, ups[::-1])
    sources = (in_hbm, cot_hbm)
    outs = (rows_in_hbm, rows_cot_hbm)
    first_slot = differ(row, place, ups)

    def span(s):
        return pl.ds(pl.multiple_of(s * part, part), part)

    def each(act):
        @pl.loop(0, SUBS)
        def _(s):
            act(s)

    def remote(src, dst, send, recv, tok, where):
        return pltpu.make_async_remote_copy(
            src_ref=src, dst_ref=dst, send_sem=send, recv_sem=recv,
            device_id=(tok, where), device_id_type=MESH,
        )

    def source_copy(a, s):
        return remote(
            sources[a].at[span(s)], rows.at[a, core, first_slot, span(s)],
            source_sem.at[a, s], own_sem.at[a, first_slot * SUBS + s],
            place, place * share + core,
        )

    def local_copy(a, s):
        return pltpu.make_async_copy(
            sources[a].at[span(s)], rows.at[a, core, 0, span(s)], own_sem.at[a, s]
        )

    def start_sources(a):
        @pl.when(row != place)
        def _():
            each(lambda s: source_copy(a, s).start())

        @pl.when(row == place)
        def _():
            each(lambda s: local_copy(a, s).start())

    def pass_copy(a, j, s, way):
        index = j * SUBS + s
        piece = rows.at[a, core, j, span(s)]
        if way < 2:
            where = (place + (1 if way else -1)) * share + core
            recv = own_sem.at[a, index]
        else:
            where = place * share + (core + way - 1) % share
            recv = mate_sem.at[a, way - 2, index]
        return remote(piece, piece, pass_sem.at[way, a, index], recv, row, where)

    to_left = jnp.logical_and(place <= row, place > 0)
    to_right = jnp.logical_and(place >= row, place < n - 1)

    def passes(a, j, s, act):
        @pl.when(to_left)
        def _():
            act(pass_copy(a, j, s, 0))

        @pl.when(to_right)
        def _():
            act(pass_copy(a, j, s, 1))

        for by in range(1, share):
            act(pass_copy(a, j, s, by + 1))

    def chain(a, j):
        def step(s):
            pltpu.make_async_copy(
                sources[a].at[span(s)], rows.at[a, core, j, span(s)], own_sem.at[a, j * SUBS + s]
            ).wait()
            passes(a, j, s, lambda copy: copy.start())

        each(step)

    def mates(a, j):
        for by in range(1, share):
            other = (core + share - by) % share

            def step(s):
                pltpu.make_async_copy(
                    sources[a].at[span(s)],
                    rows.at[a, other, j, span(s)],
                    mate_sem.at[a, by - 1, j * SUBS + s],
                ).wait()

            each(step)

    def product(m, a, j, start):
        total = None
        for c in range(share):
            term = jnp.dot(
                rows[a, c, j],
                weights[m, pl.ds(c * cols, cols), pl.ds(start, wide)],
                preferred_element_type=jnp.float32,
            )
            total = term if total is None else total + term
        return total

    def stage_of(j, bits):
        return [s for s, bit in enumerate(bits) if j & bit][0]

    def message(m, side, j):
        bit = orders[side][stage_of(j, orders[side])]
        i = m * 2 + side
        return remote(
            sent.at[i, j - 1], got.at[i, j - 1],
            sent_sem.at[i, j - 1], got_sem.at[i, j - 1], flip(row, bit), hid,
        )

    def arrivals(j, bits):
        stages = bits if j == 0 else bits[: stage_of(j, bits)]
        return [j ^ bit for bit in stages]

    def block(m, a, side, j):
        i = m * 2 + side
        came = arrivals(j, orders[side])
        for k in came:
            message(m, side, k).wait_recv()

        @pl.loop(0, half // wide)
        def _(step):
            at = pl.multiple_of(step * wide, wide)
            value = product(m, a, j, pl.multiple_of(side * half + at, wide))
            for k in came:
                value = value + got[i, k - 1, :, pl.ds(at, wide)].astype(jnp.float32)
            if j:
                sent[i, j - 1, :, pl.ds(at, wide)] = value.astype(jnp.bfloat16)
            else:
                pre_ref[m, :, pl.ds(pl.multiple_of(side * half + at, wide), wide)] = value

        if j:
            message(m, side, j).start()

    def logit_message(j):
        return remote(
            logit_sent.at[j - 1], logit_got.at[j - 1],
            logit_sent_sem.at[j - 1], logit_got_sem.at[j - 1], flip(row, ups[stage_of(j, ups)]), hid,
        )

    def logit_block(j):
        value = None
        for c in range(share):
            term = contract_cols(router_ref[:, c * cols : (c + 1) * cols], rows[0, c, j])
            value = term if value is None else value + term
        for k in arrivals(j, ups):
            logit_message(k).wait_recv()
            value = value + logit_got[k - 1]
        if j:
            logit_sent[j - 1] = value
            logit_message(j).start()
        else:
            logit_ref[...] = value

    def by_stage(stage, side):
        return [j for j in range(1, n) if stage_of(j, orders[side]) == stage]

    def pair(j, side):
        @pl.loop(0, 2)
        def _(m):
            block(m, 0, side, j)

    strips = strip.shape[1]
    count = weights.shape[1] // strips

    def strip_copy(i):
        at = pl.ds(pl.multiple_of(i * strips, strips), strips)
        return pltpu.make_async_copy(gu_hbm.at[at], strip.at[i % 2], strip_sem.at[i % 2])

    full_load = pltpu.make_async_copy(full_hbm, full, weight_sem.at[0])
    down_load = pltpu.make_async_copy(down_hbm, weights.at[2], weight_sem.at[1])
    out_cot_picked = pltpu.make_async_copy(picked, cot_hbm, weight_sem.at[2])
    out_weights = pltpu.make_async_copy(weights.at[pl.ds(0, 2)], weights_hbm, weight_sem.at[3])
    start_sources(0)
    full_load.start()
    strip_copy(0).start()
    strip_copy(1).start()
    chain(0, 0)
    full_load.wait()
    down_load.start()

    @pl.loop(0, cols // wide_pick)
    def _(step):
        at = pl.ds(pl.multiple_of(step * wide_pick, wide_pick), wide_pick)
        picked[:, at] = jnp.dot(
            one_hot_ref[...], full[:, at], preferred_element_type=jnp.float32
        ).astype(jnp.bfloat16)

    out_cot_picked.start()

    @pl.loop(0, count)
    def _(i):
        strip_copy(i).wait()
        at = pl.ds(pl.multiple_of(i * strips, strips), strips)
        for x in range(2):
            weights[x, at, :] = strip[i % 2, :, x, :]

        @pl.when(i + 2 < count)
        def _():
            strip_copy(i + 2).start()

    out_cot_picked.wait()
    start_sources(1)
    out_weights.start()
    for j in range(n):
        if j:
            chain(0, j)
        mates(0, j)
        for side in range(2):
            if j and stage_of(j, orders[side]) == 0:
                pair(j, side)
        if j and stage_of(j, ups) == 0:
            logit_block(j)
    out_in = pltpu.make_async_copy(rows.at[0], rows_in_hbm, out_sem.at[0])
    out_in.start()
    singles = [1 << b for b in range((n - 1).bit_length())]
    late = [j for j in range(1, n) if j not in singles][::-1] + singles
    for j in late[:-1]:
        chain(1, j)
    for stage in range(1, len(ups)):
        for j in by_stage(stage, 0):
            logit_block(j)
        for m in range(2):
            for side in range(2):
                for j in by_stage(stage, side):
                    block(m, 0, side, j)
            if stage == 1 and m == 0:
                chain(1, late[-1])

                @pl.when(row == place)
                def _():
                    chain(1, 0)

    down_load.wait()
    for j in late:
        mates(1, j)
        for side in range(2):
            if stage_of(j, orders[side]) == 0:
                block(2, 1, side, j)
    for stage in range(1, len(ups)):
        for side in range(2):
            for j in by_stage(stage, side):
                block(2, 1, side, j)

    @pl.when(row != place)
    def _():
        chain(1, 0)

    pair(0, 0)
    pair(0, 1)
    logit_block(0)
    mates(1, 0)
    out_cot = pltpu.make_async_copy(rows.at[1], rows_cot_hbm, out_sem.at[1])
    out_cot.start()
    for side in range(2):
        block(2, 1, side, 0)

    out_in.wait()
    out_cot.wait()
    out_weights.wait()
    for a in range(2):
        @pl.when(row != place)
        def _():
            each(lambda s: source_copy(a, s).wait_send())

        for j in range(n):
            each(lambda s: passes(a, j, s, lambda copy: copy.wait_send()))
    for j in range(1, n):
        logit_message(j).wait_send()
        for side in range(2):
            for m in range(3):
                message(m, side, j).wait_send()


def forward_call(n, share, picked_in, cotangent, one_hot, router_cols, gate_up, down):
    slots, cols = picked_in.shape
    depth, hidden = down.shape
    experts = router_cols.shape[0]
    half = hidden // 2
    hbm = pl.BlockSpec(memory_space=pltpu.HBM)
    vmem = pl.BlockSpec(memory_space=pltpu.VMEM)
    spread = (share, n, slots, cols)
    dma = pltpu.SemaphoreType.DMA
    return pl.pallas_call(
        functools.partial(forward_kernel, n, share),
        in_specs=[hbm, hbm, vmem, vmem, hbm, hbm],
        out_specs=[hbm, hbm, hbm, hbm, vmem, vmem],
        out_shape=[
            jax.ShapeDtypeStruct(spread, jnp.bfloat16),
            jax.ShapeDtypeStruct(spread, jnp.bfloat16),
            jax.ShapeDtypeStruct((slots, cols), jnp.bfloat16),
            jax.ShapeDtypeStruct((2, depth, hidden), jnp.bfloat16),
            jax.ShapeDtypeStruct((3, slots, hidden), jnp.float32),
            jax.ShapeDtypeStruct((experts, slots), jnp.float32),
        ],
        scratch_shapes=[
            pltpu.VMEM((2, *spread), jnp.bfloat16),
            pltpu.VMEM((3, depth, hidden), jnp.bfloat16),
            pltpu.VMEM(cotangent.shape, jnp.bfloat16),
            pltpu.VMEM((slots, cols), jnp.bfloat16),
            pltpu.VMEM((2, depth // 12, 2, hidden), jnp.bfloat16),
            pltpu.VMEM((6, n - 1, slots, half), jnp.bfloat16),
            pltpu.VMEM((6, n - 1, slots, half), jnp.bfloat16),
            pltpu.VMEM((n - 1, experts, slots), jnp.float32),
            pltpu.VMEM((n - 1, experts, slots), jnp.float32),
            dma((2, SUBS)),
            dma((2, n * SUBS)),
            dma((2, share - 1, n * SUBS)),
            dma((share + 1, 2, n * SUBS)),
            dma((4,)),
            dma((2,)),
            dma((6, n - 1)),
            dma((6, n - 1)),
            dma((n - 1,)),
            dma((n - 1,)),
            dma((2,)),
        ],
        compiler_params=pltpu.CompilerParams(vmem_limit_bytes=60 * 2**20, has_side_effects=True),
        cost_estimate=pl.CostEstimate(
            flops=6 * n * slots * depth * hidden, bytes_accessed=60 * 2**20, transcendentals=0
        ),
        name="forward",
    )(picked_in, cotangent, one_hot, router_cols, gate_up, down)


def backward_kernel(
    n, share, tile,
    grads_hbm, score_ref, weights_hbm, rows_in_hbm, rows_cot_hbm,
    back_ref, score_out_ref, pair_hbm, down_hbm,
    grads, weights, rows, kept, mate_sent, mate_got, flow_got, flow_sent, flow_sum, last_got,
    pair_tile, down_tile, score_got,
    load_sem, grad_sent_sem, grad_got_sem, mate_sent_sem, mate_got_sem, flow_sent_sem, flow_got_sem,
    last_sem, tile_sem, score_sent_sem, score_got_sem,
):
    row = lax.axis_index("tok")
    hid = lax.axis_index("hid")
    n_hid = n * share
    place = hid // share
    core = hid % share
    slots, hidden = grads.shape[2:]
    cols = rows.shape[4]
    half = hidden // 2
    part = slots // SUBS
    per = cols // tile
    bits = [1 << b for b in range((n - 1).bit_length())]
    singles = [j for j in range(1, n) if j in bits]
    others = sorted((j for j in range(1, n) if j not in bits), key=lambda j: bin(j).count("1"))

    def remote(src, dst, send, recv, tok, where):
        return pltpu.make_async_remote_copy(
            src_ref=src, dst_ref=dst, send_sem=send, recv_sem=recv,
            device_id=(tok, where), device_id_type=MESH,
        )

    def route(j, side):
        through = [bit for bit in bits if j & bit]
        return through[-1] if side else through[0]

    def grad_message(x, j, side):
        bit = route(j, side)
        columns = pl.ds(side * half, half)
        return remote(
            grads.at[x, j ^ bit, :, columns], grads.at[x, j, :, columns],
            grad_sent_sem.at[x, j - 1, side], grad_got_sem.at[x, j - 1, side], flip(row, bit), hid,
        )

    def direct(x):
        for j in singles:
            for side in range(2):
                grad_message(x, j, side).start()

    def onward(x, source):
        for j in others:
            for side in range(2):
                if j ^ route(j, side) == source:
                    grad_message(x, j, side).start()

    def take(x, j):
        for side in range(2):
            grad_message(x, j, side).wait_recv()
        onward(x, j)

    def mate_copy(j, by):
        return remote(
            mate_sent.at[by - 1, j], mate_got.at[by - 1, j],
            mate_sent_sem.at[by - 1, j], mate_got_sem.at[by - 1, j],
            row, place * share + (core + by) % share,
        )

    def back_tile(j, start):
        total = None
        for x in range(2):
            term = contract_cols(grads[x, j], weights[x, pl.ds(start, tile), :])
            total = term if total is None else total + term
        return total

    def back(j):
        for by in range(share - 1, -1, -1):
            base = (core + by) % share * cols

            @pl.loop(0, per)
            def _(step):
                at = pl.multiple_of(step * tile, tile)
                value = back_tile(j, pl.multiple_of(base + at, tile))
                if by:
                    mate_sent[by - 1, j, :, pl.ds(at, tile)] = value.astype(jnp.bfloat16)
                else:
                    kept[j, :, pl.ds(at, tile)] = value

            if by:
                mate_copy(j, by).start()

    from_left = jnp.logical_and(place <= row, place > 0)
    from_right = jnp.logical_and(place >= row, place < n - 1)

    def span(s):
        return pl.ds(pl.multiple_of(s * part, part), part)

    def flow_copy(j, s, way):
        return remote(
            flow_sent.at[j, span(s)], flow_got.at[way, j, span(s)],
            flow_sent_sem.at[j, s], flow_got_sem.at[way, j, s],
            row, (place + (-1 if way else 1)) * share + core,
        )

    def last_copy(j, s):
        tok = row
        for bit in bits:
            if j & bit:
                tok = flip(tok, bit)
        return remote(
            flow_sent.at[j, span(s)], last_got.at[span(s)],
            flow_sent_sem.at[j, s], last_sem.at[s], tok, hid,
        )

    def flow_moves(j, s, act):
        @pl.when(place < row)
        def _():
            act(flow_copy(j, s, 0))

        @pl.when(place > row)
        def _():
            act(flow_copy(j, s, 1))

        if j:
            @pl.when(place == row)
            def _():
                act(last_copy(j, s))

    def flow(j, s):
        value = kept[j, span(s)]
        for by in range(1, share):
            value = value + mate_got[by - 1, j, span(s)].astype(jnp.float32)
        flow_sum[...] = value
        for way, present in enumerate((from_left, from_right)):
            @pl.when(present)
            def _():
                flow_copy(j, s, way).wait_recv()
                flow_sum[...] += flow_got[way, j, span(s)].astype(jnp.float32)

        flow_sent[j, span(s)] = flow_sum[...].astype(jnp.bfloat16)
        if j == 0:
            @pl.when(place == row)
            def _():
                back_ref[span(s)] = flow_sum[...].astype(jnp.bfloat16)

        flow_moves(j, s, lambda copy: copy.start())

    def mates(j):
        for by in range(1, share):
            mate_copy(j, by).wait_recv()

    def flows(j):
        mates(j)

        @pl.loop(0, SUBS)
        def _(s):
            flow(j, s)

    def tile_copy(x, i):
        slot = i % 2
        at = pl.ds(pl.multiple_of(i * tile, tile), tile)
        if x:
            return pltpu.make_async_copy(down_tile.at[slot], down_hbm.at[at], tile_sem.at[1, slot])
        return pltpu.make_async_copy(pair_tile.at[slot], pair_hbm.at[at], tile_sem.at[0, slot])

    def tile_sum(a, x, i):
        at = pl.ds(pl.multiple_of(i % per * tile, tile), tile)
        total = None
        for j in range(n):
            term = contract_rows(rows[a, i // per, j, :, at], grads[x, j])
            total = term if total is None else total + term
        return total

    def pair_step(i):
        @pl.when(i >= 2)
        def _():
            tile_copy(0, i - 2).wait()

        for x in range(2):
            pair_tile[i % 2, :, x, :] = tile_sum(0, x, i)
        tile_copy(0, i).start()

    def down_step(i):
        @pl.when(i >= 2)
        def _():
            tile_copy(1, i - 2).wait()

        down_tile[i % 2] = tile_sum(1, 2, i)
        tile_copy(1, i).start()

    def score_copy(by):
        return remote(
            score_ref, score_got.at[by - 1],
            score_sent_sem.at[by - 1], score_got_sem.at[by - 1], row, (hid + by) % n_hid,
        )

    own_loads = [pltpu.make_async_copy(grads_hbm.at[x], grads.at[x, 0], load_sem.at[x]) for x in range(3)]
    weight_load = pltpu.make_async_copy(weights_hbm, weights, load_sem.at[3])
    row_loads = [
        pltpu.make_async_copy(rows_in_hbm, rows.at[0], load_sem.at[4]),
        pltpu.make_async_copy(rows_cot_hbm, rows.at[1], load_sem.at[5]),
    ]
    for load in own_loads:
        load.start()
    weight_load.start()
    for x in range(2):
        own_loads[x].wait()
        direct(x)
    for by in range(1, n_hid):
        score_copy(by).start()
    weight_load.wait()
    for load in row_loads:
        load.start()
    back(0)
    flows(0)
    own_loads[2].wait()
    for x in range(2):
        for j in singles:
            take(x, j)
    direct(2)
    for j in singles:
        back(j)
        flows(j)
    for j in others[:-1]:
        for x in range(2):
            take(x, j)
        back(j)
        flows(j)
    end = others[-1]
    for x in range(2):
        take(x, end)
    back(end)
    mates(end)
    for load in row_loads:
        load.wait()
    for j in singles:
        take(2, j)
    tiles = share * per
    each = -(-tiles // SUBS)

    @pl.loop(0, SUBS)
    def _(s):
        @pl.loop(0, each)
        def _(step):
            @pl.when(s * each + step < tiles)
            def _():
                pair_step(s * each + step)

        flow(end, s)

    for j in others:
        take(2, j)

    @pl.loop(0, tiles)
    def _(i):
        down_step(i)

    total = score_ref[...]
    for by in range(1, n_hid):
        score_copy(by).wait_recv()
        total = total + score_got[by - 1]
    score_out_ref[...] = total

    @pl.when(place != row)
    def _():
        @pl.loop(0, SUBS)
        def _(s):
            last_copy(1, s).wait_recv()

        back_ref[...] = last_got[...]

    for i in range(max(0, tiles - 2), tiles):
        for x in range(2):
            tile_copy(x, i).wait()
    for by in range(1, n_hid):
        score_copy(by).wait_send()
    for x in range(3):
        for j in range(1, n):
            for side in range(2):
                grad_message(x, j, side).wait_send()
    for j in range(n):
        for by in range(1, share):
            mate_copy(j, by).wait_send()

        @pl.loop(0, SUBS)
        def _(s):
            flow_moves(j, s, lambda copy: copy.wait_send())


def backward_call(n, share, own, scores, weights, rows_in, rows_cot):
    _, slots, hidden = own.shape
    cols = rows_in.shape[3]
    depth = share * cols
    tile = 256 if cols % 256 == 0 else 128
    part = slots // SUBS
    n_hid = n * share
    hbm = pl.BlockSpec(memory_space=pltpu.HBM)
    vmem = pl.BlockSpec(memory_space=pltpu.VMEM)
    dma = pltpu.SemaphoreType.DMA
    half = jnp.bfloat16
    return pl.pallas_call(
        functools.partial(backward_kernel, n, share, tile),
        in_specs=[hbm, vmem, hbm, hbm, hbm],
        out_specs=[vmem, vmem, hbm, hbm],
        out_shape=[
            jax.ShapeDtypeStruct((slots, cols), half),
            jax.ShapeDtypeStruct(scores.shape, jnp.float32),
            jax.ShapeDtypeStruct((depth, 2, hidden), jnp.float32),
            jax.ShapeDtypeStruct((depth, hidden), jnp.float32),
        ],
        scratch_shapes=[
            pltpu.VMEM((3, n, slots, hidden), half),
            pltpu.VMEM((2, depth, hidden), half),
            pltpu.VMEM((2, share, n, slots, cols), half),
            pltpu.VMEM((n, slots, cols), jnp.float32),
            pltpu.VMEM((share - 1, n, slots, cols), half),
            pltpu.VMEM((share - 1, n, slots, cols), half),
            pltpu.VMEM((2, n, slots, cols), half),
            pltpu.VMEM((n, slots, cols), half),
            pltpu.VMEM((part, cols), jnp.float32),
            pltpu.VMEM((slots, cols), half),
            pltpu.VMEM((2, tile, 2, hidden), jnp.float32),
            pltpu.VMEM((2, tile, hidden), jnp.float32),
            pltpu.VMEM((n_hid - 1, *scores.shape), jnp.float32),
            dma((6,)),
            dma((3, n - 1, 2)),
            dma((3, n - 1, 2)),
            dma((share - 1, n)),
            dma((share - 1, n)),
            dma((n, SUBS)),
            dma((2, n, SUBS)),
            dma((SUBS,)),
            dma((2, 2)),
            dma((n_hid - 1,)),
            dma((n_hid - 1,)),
        ],
        compiler_params=pltpu.CompilerParams(vmem_limit_bytes=63 * 2**20, has_side_effects=True),
        cost_estimate=pl.CostEstimate(
            flops=10 * n * slots * depth * hidden, bytes_accessed=60 * 2**20, transcendentals=0
        ),
        name="backward",
    )(own, scores, weights, rows_in, rows_cot)


def local(tokens, cotangent, expert_choice, router, gate_up, w_down):
    n_tok = lax.axis_size("tok")
    n_hid = lax.axis_size("hid")
    share = n_hid // n_tok
    weight_rows = w_down.shape[0]
    row = lax.axis_index("tok")
    first = expert_choice[:, 0]
    second = expert_choice[:, 1]
    in_first = first == 0
    in_second = second == 0
    routed = jnp.logical_or(in_first, in_second)
    flags = routed.astype(jnp.int32)
    slot_rank = jnp.cumsum(flags) - flags
    slot_ids = jnp.arange(CAP, dtype=jnp.int32)
    placed = jnp.logical_and(routed[None, :], slot_rank[None, :] == slot_ids[:, None])
    one_hot = placed.astype(jnp.bfloat16)
    def pick(values):
        return jnp.dot(one_hot, values, preferred_element_type=jnp.float32).astype(jnp.bfloat16)

    router_cols = lax.dynamic_slice_in_dim(router, row * weight_rows, weight_rows, 1)
    pieces_in, pieces_cot, _, weights, pre, logits = forward_call(
        n_tok, share, pick(tokens), cotangent, one_hot, router_cols, gate_up, w_down
    )
    gate_pre, up_pre, raw = pre[0], pre[1], pre[2]
    slot_other = jnp.sum(jnp.where(placed, (first + second)[None, :], 0), axis=1)
    filled = jnp.any(placed, axis=1)
    labels = jnp.arange(logits.shape[0], dtype=jnp.int32)
    other_logit = jnp.sum(jnp.where(slot_other[None, :] == labels[:, None], logits, 0.0), axis=0)
    slot_gate = jnp.where(filled, jax.nn.sigmoid(logits[0] - other_logit), 0.0)

    active, slope = silu_pair(gate_pre)
    product = active * up_pre
    scale = slot_gate[:, None]
    score_part = jnp.sum(product * raw, axis=1)
    upstream = scale * raw
    own = jnp.stack(
        [
            (upstream * up_pre * slope).astype(jnp.bfloat16),
            (upstream * active).astype(jnp.bfloat16),
            (scale * product).astype(jnp.bfloat16),
        ]
    )
    back_cols, scores, d_gate_up, d_down = backward_call(
        n_tok, share, own, score_part[None, :], weights, pieces_in, pieces_cot
    )
    scores = scores[0]
    grad_tokens = contract_rows(one_hot, back_cols).astype(jnp.bfloat16)
    token_score = jnp.sum(jnp.where(placed, scores[:, None], 0.0), axis=0)
    d_combine = jnp.stack(
        [jnp.where(in_first, token_score, 0.0), jnp.where(in_second, token_score, 0.0)], axis=1
    )
    return (grad_tokens, d_combine, d_gate_up, d_down)


def solution(mesh):
    in_specs = (
        P("tok", "hid"),
        P("tok", "hid"),
        P("tok", None),
        P(),
        P("tok", None, "hid"),
        P("tok", "hid"),
    )
    out_specs = (P("tok", "hid"), P("tok", None), P("tok", None, "hid"), P("tok", "hid"))
    return jax.shard_map(local, mesh=mesh, in_specs=in_specs, out_specs=out_specs, check_vma=False)
```
